32 devices in a mesh: dp: 2 (over x), vocab: 16 (over z, y, core).
Axes of the slice: x: 2, y: 2, z: 4, core: 2. Of those that a mesh axis runs over, the one named last changes fastest.
Arguments:
- hidden: bfloat16 [160, 4608], P('dp'), may hold values from -30 to 30
- head_weight: bfloat16 [4608, 16384], P(None, ('dp', 'vocab')), may hold values from -0.09375 to 0.09375
- drafts: int32 [32, 4], replicated, may hold values from 0 to 16383
- cutoffs: int32 [32, 4], P('dp'), may hold values from -30720 to -18433
Outputs:
- log_norm: float32 [32, 5], P('dp')
- draft_logprob: float32 [32, 4], P('dp')
- expected_accept: float32 [32], P('dp')
- z_loss: float32 [], replicated
The draws below stay inside these ranges and needn't reach their ends.
All inputs are finite; a program needn't handle non-finite values.
Results may differ from the reference program's by a relative error of at most 0.0003.
Values may be sent and summed in bfloat16 or wider, within the bound.
No kernel may reach another device: no remote copies, remote signals or barrier semaphores. Data moves between devices by JAX's collectives and lax.ppermute only.
A program may use at most 64 MiB of HBM per device.

```python
import jax
import jax.numpy as jnp
from jax import lax

D = 4608
V_DEV = 512
DRAFTS = 4
POSITIONS = 5
SEQS = 32
VOCAB = 16384
N_DP = 2
N_VOCAB = 16


def plant(result, key, low, largest):
    longest = result.shape.index(max(result.shape))
    spots = []
    for shift in (0, 1):
        where = [jax.random.randint(jax.random.fold_in(key, axis), (), 0, length) for axis, length in enumerate(result.shape)]
        where[longest] = (where[longest] + shift) % result.shape[longest]
        spots.append(tuple(where))
    return result.at[spots[0]].set(low).at[spots[1]].set(largest)


def block_scale(own_key, shape, shards, smallest, largest):
    def one(position, blocks):
        heights = jax.random.uniform(jax.random.fold_in(jax.random.fold_in(own_key, 6), position), (blocks,), jnp.float32, smallest / len(shards), largest / len(shards))
        return jnp.repeat(jnp.exp(heights), shape[position] // blocks).reshape((-1,) + (1,) * (len(shape) - position - 1))

    factor_of = one(*shards[0])
    for cut in shards[1:]:
        factor_of = factor_of * one(*cut)
    return factor_of


def normal_values(stream_key, extent, spread, most, pieces=(), kind=jnp.bfloat16):
    values = spread * jax.random.normal(stream_key, extent, jnp.float32)
    if pieces:
        values = values * block_scale(stream_key, extent, pieces, -0.22, 0.18)
    return jnp.clip(values, -most, most).astype(kind)


def setup_inputs(seed: int = 0) -> dict:
    keys = jax.random.split(jax.random.key(seed), 5)
    return {
        "hidden": normal_values(keys[0], (SEQS * POSITIONS, D), 5.0, 30.0, ((0, 2),)),
        "head_weight": normal_values(keys[1], (D, VOCAB), D ** -0.5, 0.09375, ((1, 32),)),
        "drafts": plant(jax.random.randint(keys[2], (SEQS, DRAFTS), 0, VOCAB), jax.random.fold_in(keys[2], 1), 0, VOCAB - 1).astype(jnp.int32),
        "cutoffs": plant(jax.random.randint(keys[3], (SEQS, DRAFTS), -30720, -18432), jax.random.fold_in(keys[3], 1), -30720, (-18432) - 1).astype(jnp.int32),
    }


SOFT_CAP = 30.0
Z_WEIGHT = 0.001


def reference(hidden, head_weight, drafts, cutoffs):
    stride = V_DEV * N_VOCAB
    sentinel = jnp.full((drafts.shape[0], 1), -1, jnp.int32)
    draft_rows = jnp.concatenate([drafts, sentinel], axis=1).reshape(-1)
    columns = lax.broadcasted_iota(jnp.int32, (1, stride), 1)

    def accumulate(carry, block):
        exp_total, picked = carry
        weights = lax.dynamic_slice_in_dim(head_weight, (block * stride).astype(jnp.int32), stride, 1)
        logits = jnp.dot(hidden, weights, preferred_element_type=jnp.float32)
        capped = SOFT_CAP * jnp.tanh(logits / SOFT_CAP)
        exp_total = exp_total + jnp.sum(jnp.exp(capped), axis=1)
        target = draft_rows - (block * stride).astype(jnp.int32)
        picked = picked + jnp.sum(jnp.where(columns == target[:, None], capped, jnp.zeros_like(capped)), axis=1)
        return (exp_total, picked), None

    zeros = jnp.zeros((hidden.shape[0],), jnp.float32)
    (exp_total, picked), unused = lax.scan(accumulate, (zeros, zeros), jnp.arange(N_DP, dtype=jnp.int32))
    log_total = jnp.log(exp_total)
    z_loss = Z_WEIGHT * jnp.mean(log_total * log_total)
    log_norm = log_total.reshape(-1, POSITIONS)
    picks = picked.reshape(-1, POSITIONS)
    draft_logprob = picks[:, :DRAFTS] - log_norm[:, :DRAFTS]
    accept = jax.nn.sigmoid(draft_logprob - cutoffs.astype(jnp.float32) / 1024.0)
    expected_accept = jnp.sum(jnp.cumprod(accept, axis=1), axis=1)
    return log_norm, draft_logprob, expected_accept, z_loss
```

```python
import functools

import jax
import jax.numpy as jnp
from jax import lax
from jax.experimental import pallas as pl
from jax.experimental.pallas import tpu as pltpu
from jax.sharding import PartitionSpec as P

DRAFTS = 4
POSITIONS = 5
SOFT_CAP = 30.0
Z_WEIGHT = 0.001
LANES = 128
GRANT = 16 * 2**20
VMEM = pl.BlockSpec(memory_space=pltpu.VMEM)


def tile_width(seqs):
    return -(-2 * seqs // LANES) * LANES


def row_ids(drafts, rows, first_seq):
    shape = (rows, drafts.shape[1])
    seq = lax.broadcasted_iota(jnp.int32, shape, 1) - first_seq
    target = lax.broadcasted_iota(jnp.int32, shape, 0) - seq * POSITIONS
    shifted = (drafts + 1).astype(jnp.float32)
    picked = jnp.zeros(shape, jnp.float32)
    for p in range(DRAFTS):
        picked = jnp.where(target == p, shifted[p : p + 1], picked)
    return jnp.sum(picked, axis=1, keepdims=True).astype(jnp.int32) - 1


def contribution(logits, drafts, first_seq):
    rows, width = logits.shape
    seqs = drafts.shape[1]
    shard = lax.axis_index("dp") * lax.axis_size("vocab") + lax.axis_index("vocab")
    ids = row_ids(drafts, rows, first_seq) - shard * width
    capped = SOFT_CAP * jnp.tanh(logits * (1.0 / SOFT_CAP))
    totals = jnp.sum(jnp.exp(capped), axis=1, keepdims=True)
    columns = lax.broadcasted_iota(jnp.int32, (rows, width), 1)
    picks = jnp.sum(jnp.where(columns == ids, capped, 0.0), axis=1, keepdims=True)
    shape = (rows, tile_width(seqs))
    lane = lax.broadcasted_iota(jnp.int32, shape, 1)
    row = lax.broadcasted_iota(jnp.int32, shape, 0)
    values = jnp.where(lane < seqs, totals, picks)
    seq = jnp.where(lane < seqs, lane, lane - seqs) - first_seq
    target = row - seq * POSITIONS
    position = lax.broadcasted_iota(jnp.int32, (8, shape[1]), 0)
    tile = jnp.zeros((8, shape[1]), jnp.float32)
    for p in range(POSITIONS):
        line = jnp.sum(jnp.where(target == p, values, 0.0), axis=0, keepdims=True)
        tile = jnp.where(position == p, line, tile)
    return tile


def own_kernel(hidden_ref, weight_ref, drafts_ref, tile_ref):
    own_seqs = hidden_ref.shape[0] // POSITIONS
    first_seq = lax.axis_index("dp") * own_seqs
    logits = jnp.dot(hidden_ref[...], weight_ref[...], preferred_element_type=jnp.float32)
    tile_ref[...] = contribution(logits, drafts_ref[...], first_seq)


def other_kernel(shift, copies, near_ref, far_ref, weight_ref, drafts_ref, before_ref, out_ref):
    own_seqs = near_ref.shape[0] // POSITIONS
    dp = lax.axis_size("dp")
    source = lax.rem(lax.axis_index("dp") + dp - shift, dp)
    depth = near_ref.shape[1]
    core = lax.rem(lax.axis_index("vocab"), 2)
    near = pl.ds(pl.multiple_of(core * depth, depth), depth)
    far = pl.ds(pl.multiple_of((1 - core) * depth, depth), depth)
    logits = jnp.dot(near_ref[...], weight_ref[near, :], preferred_element_type=jnp.float32)
    logits += jnp.dot(far_ref[...], weight_ref[far, :], preferred_element_type=jnp.float32)
    tile = contribution(logits, drafts_ref[...], source * own_seqs) + before_ref[...]
    out_ref[...] = jnp.broadcast_to(tile[None], (copies,) + tile.shape)


def tail_kernel(seqs, parts_ref, cutoffs_ref, norm_ref, logprob_ref, expected_ref, loss_ref):
    own_seqs = cutoffs_ref.shape[1]
    width = parts_ref.shape[2]
    tile = jnp.sum(parts_ref[...], axis=0)
    position = lax.broadcasted_iota(jnp.int32, tile.shape, 0)
    lane = lax.broadcasted_iota(jnp.int32, tile.shape, 1)
    log_total = jnp.log(jnp.where((position < POSITIONS) & (lane < seqs), tile, 1.0))
    squares = jnp.sum(jnp.sum(log_total * log_total, axis=1, keepdims=True), axis=0, keepdims=True)
    loss_ref[...] = squares * (Z_WEIGHT / (seqs * POSITIONS))
    first = lax.axis_index("dp") * own_seqs
    log_norm = pltpu.roll(log_total, lax.rem(width - first, width), 1)
    picks = pltpu.roll(tile, lax.rem(2 * width - seqs - first, width), 1)
    norm_ref[...] = log_norm[:POSITIONS, :own_seqs]
    logprob = picks[:DRAFTS, :own_seqs] - log_norm[:DRAFTS, :own_seqs]
    logprob_ref[...] = logprob
    accept = jax.nn.sigmoid(logprob - cutoffs_ref[...].astype(jnp.float32) / 1024.0)
    product = accept[0:1]
    expected = product
    for p in range(1, DRAFTS):
        product = product * accept[p : p + 1]
        expected = expected + product
    expected_ref[...] = expected


def local(hidden, head_weight, drafts, cutoffs):
    dp, vocab = lax.axis_size("dp"), lax.axis_size("vocab")
    rows, depth = hidden.shape
    width = head_weight.shape[1]
    seqs = drafts.shape[0]
    own_seqs = rows // POSITIONS
    tile = jax.ShapeDtypeStruct((8, tile_width(seqs)), jnp.float32)
    half = depth // 2
    core = lax.rem(lax.axis_index("vocab"), 2)
    mine = lax.dynamic_slice_in_dim(hidden, core * half, half, 1)
    swap = [(i, i ^ 1) for i in range(vocab)]
    near = [lax.ppermute(mine, "dp", [(i, (i + k) % dp) for i in range(dp)]) for k in range(1, dp)]
    cost = pl.CostEstimate(
        flops=2 * rows * depth * width,
        bytes_accessed=2 * depth * (rows + width),
        transcendentals=2 * rows * width,
    )
    tokens = drafts.T
    parts = pl.pallas_call(
        own_kernel,
        out_shape=tile,
        in_specs=[VMEM] * 3,
        out_specs=VMEM,
        cost_estimate=cost,
        compiler_params=pltpu.CompilerParams(vmem_limit_bytes=GRANT),
        name="own_rows",
    )(hidden, head_weight, tokens)
    near, parts = lax.optimization_barrier((near, parts))
    far = [lax.ppermute(block, "vocab", swap) for block in near]
    for k in range(1, dp):
        copies = dp * vocab if k == dp - 1 else 1
        parts = pl.pallas_call(
            functools.partial(other_kernel, k, copies),
            out_shape=jax.ShapeDtypeStruct((copies,) + tile.shape, jnp.float32),
            in_specs=[VMEM] * 5,
            out_specs=VMEM,
            cost_estimate=cost,
            compiler_params=pltpu.CompilerParams(vmem_limit_bytes=GRANT),
            name="other_rows",
        )(near[k - 1], far[k - 1], head_weight, tokens, parts)
        if copies == 1:
            parts = parts[0]
    parts = lax.all_to_all(parts, ("dp", "vocab"), 0, 0)
    log_norm, logprob, expected, loss = pl.pallas_call(
        functools.partial(tail_kernel, seqs),
        out_shape=(
            jax.ShapeDtypeStruct((POSITIONS, own_seqs), jnp.float32),
            jax.ShapeDtypeStruct((DRAFTS, own_seqs), jnp.float32),
            jax.ShapeDtypeStruct((1, own_seqs), jnp.float32),
            jax.ShapeDtypeStruct((1, 1), jnp.float32),
        ),
        in_specs=[VMEM] * 2,
        out_specs=(VMEM,) * 4,
        compiler_params=pltpu.CompilerParams(vmem_limit_bytes=GRANT),
        name="tail",
    )(parts, cutoffs.T)
    return log_norm.T, logprob.T, expected.reshape(own_seqs), loss.reshape(())


def solution(mesh):
    in_specs = (P("dp", None), P(None, ("dp", "vocab")), P(), P("dp", None))
    out_specs = (P("dp", None), P("dp", None), P("dp"), P())
    return jax.shard_map(local, mesh=mesh, in_specs=in_specs, out_specs=out_specs, check_vma=False)
```

```python
import functools

import jax
import jax.numpy as jnp
from jax import lax
from jax.experimental import pallas as pl
from jax.experimental.pallas import tpu as pltpu
from jax.sharding import PartitionSpec as P

DRAFTS = 4
POSITIONS = 5
SOFT_CAP = 30.0
Z_WEIGHT = 0.001
LANES = 128
GRANT = 16 * 2**20
VMEM = pl.BlockSpec(memory_space=pltpu.VMEM)


def row_ids(drafts, rows, first_seq):
    shape = (rows, drafts.shape[1])
    seq = lax.broadcasted_iota(jnp.int32, shape, 1) - first_seq
    target = lax.broadcasted_iota(jnp.int32, shape, 0) - seq * POSITIONS
    shifted = (drafts + 1).astype(jnp.float32)
    picked = jnp.zeros(shape, jnp.float32)
    for p in range(DRAFTS):
        picked = jnp.where(target == p, shifted[p : p + 1], picked)
    return jnp.sum(picked, axis=1, keepdims=True).astype(jnp.int32) - 1


def spread(column, starts, lines):
    shape = (column.shape[0], LANES)
    offset = lax.broadcasted_iota(jnp.int32, shape, 0) - POSITIONS * lax.broadcasted_iota(jnp.int32, shape, 1)
    out = []
    for line in range(lines):
        values = jnp.zeros(shape, jnp.float32)
        for p, start in enumerate(starts):
            values = jnp.where(offset == POSITIONS * (line * LANES - start) + p, column, values)
        out.append(jnp.sum(values, axis=0, keepdims=True))
    return jnp.concatenate(out, axis=0)


def payload_lines(seqs, own_seqs):
    return -(-(POSITIONS * seqs + DRAFTS * own_seqs) // LANES)


def contribution(logits, drafts, source):
    rows, width = logits.shape
    seqs, own_seqs = drafts.shape[1], rows // POSITIONS
    shard = lax.axis_index("dp") * lax.axis_size("vocab") + lax.axis_index("vocab")
    ids = row_ids(drafts, rows, source * own_seqs) - shard * width
    capped = SOFT_CAP * jnp.tanh(logits * (1.0 / SOFT_CAP))
    totals = jnp.sum(jnp.exp(capped), axis=1, keepdims=True)
    columns = lax.broadcasted_iota(jnp.int32, (rows, width), 1)
    picks = jnp.sum(jnp.where(columns == ids, capped, 0.0), axis=1, keepdims=True)
    lines = payload_lines(seqs, own_seqs)
    totals = spread(totals, [p * seqs + source * own_seqs for p in range(POSITIONS)], lines)
    picks = spread(picks, [POSITIONS * seqs + p * own_seqs for p in range(DRAFTS)], lines)
    return totals, picks


def parts_for(receiver, source, totals, picks):
    return totals + jnp.where(source == receiver, picks, 0.0)


def half_kernel(hidden_ref, half_ref, done):
    depth = half_ref.shape[1]
    start = pl.multiple_of(lax.rem(lax.axis_index("vocab"), 2) * depth, depth)
    copy = pltpu.make_async_copy(hidden_ref.at[:, pl.ds(start, depth)], half_ref, done)
    copy.start()
    copy.wait()


def own_kernel(hidden_ref, weight_ref, drafts_ref, parts_ref):
    logits = jnp.dot(hidden_ref[...], weight_ref[...], preferred_element_type=jnp.float32)
    me = lax.axis_index("dp")
    totals, picks = contribution(logits, drafts_ref[...], me)
    for receiver in range(parts_ref.shape[0]):
        parts_ref[receiver] = parts_for(receiver, me, totals, picks)


def near_kernel(near_ref, weight_ref, logits_ref):
    depth = near_ref.shape[1]
    start = pl.multiple_of(lax.rem(lax.axis_index("vocab"), 2) * depth, depth)
    logits_ref[...] = jnp.dot(near_ref[...], weight_ref[pl.ds(start, depth), :], preferred_element_type=jnp.float32)


def far_kernel(shift, far_ref, weight_ref, logits_ref, drafts_ref, before_ref, parts_ref):
    depth = far_ref.shape[1]
    dp = before_ref.shape[0]
    copies = parts_ref.shape[0] // dp
    source = lax.rem(lax.axis_index("dp") + dp - shift, dp)
    start = pl.multiple_of((1 - lax.rem(lax.axis_index("vocab"), 2)) * depth, depth)
    logits = logits_ref[...] + jnp.dot(
        far_ref[...], weight_ref[pl.ds(start, depth), :], preferred_element_type=jnp.float32
    )
    totals, picks = contribution(logits, drafts_ref[...], source)
    for receiver in range(dp):
        part = before_ref[receiver] + parts_for(receiver, source, totals, picks)
        parts_ref[receiver * copies : (receiver + 1) * copies] = jnp.broadcast_to(part[None], (copies,) + part.shape)


def gather_rows(flat, starts, count):
    lines = flat.shape[0]
    lane = lax.broadcasted_iota(jnp.int32, (1, LANES), 1)
    out = []
    for low, high, start in starts:
        row = jnp.zeros((1, LANES), jnp.float32)
        for line in range(low // LANES, min(lines, (high - 1) // LANES + 1)):
            place = start - line * LANES
            moved = pltpu.roll(flat, lax.rem(lines * LANES - place, LANES), 1)[line : line + 1]
            row = jnp.where((lane + place >= 0) & (lane + place < LANES), moved, row)
        out.append(row[:, :count])
    return jnp.concatenate(out, axis=0)


def tail_kernel(seqs, parts_ref, cutoffs_ref, norm_ref, logprob_ref, expected_ref, loss_ref):
    own_seqs = cutoffs_ref.shape[1]
    flat = jnp.sum(parts_ref[...], axis=0)
    place = lax.broadcasted_iota(jnp.int32, flat.shape, 0) * LANES + lax.broadcasted_iota(jnp.int32, flat.shape, 1)
    log_total = jnp.log(jnp.where(place < POSITIONS * seqs, flat, 1.0))
    squares = jnp.sum(jnp.sum(log_total * log_total, axis=1, keepdims=True), axis=0, keepdims=True)
    loss_ref[...] = squares * (Z_WEIGHT / (seqs * POSITIONS))
    first = lax.axis_index("dp") * own_seqs
    ranges = [(p * seqs, (p + 1) * seqs, p * seqs + first) for p in range(POSITIONS)]
    log_norm = gather_rows(log_total, ranges, own_seqs)
    base = POSITIONS * seqs
    ranges = [(base + p * own_seqs, base + (p + 1) * own_seqs, base + p * own_seqs) for p in range(DRAFTS)]
    picks = gather_rows(flat, ranges, own_seqs)
    norm_ref[...] = log_norm
    logprob = picks - log_norm[:DRAFTS]
    logprob_ref[...] = logprob
    accept = jax.nn.sigmoid(logprob - cutoffs_ref[...].astype(jnp.float32) / 1024.0)
    product = accept[0:1]
    expected = product
    for p in range(1, DRAFTS):
        product = product * accept[p : p + 1]
        expected = expected + product
    expected_ref[...] = expected


def local(hidden, head_weight, drafts, cutoffs):
    dp, vocab = lax.axis_size("dp"), lax.axis_size("vocab")
    rows, depth = hidden.shape
    width = head_weight.shape[1]
    seqs, own_seqs = drafts.shape[0], rows // POSITIONS
    half = depth // 2
    lines = payload_lines(seqs, own_seqs)
    params = pltpu.CompilerParams(vmem_limit_bytes=GRANT)
    cost = pl.CostEstimate(
        flops=2 * rows * depth * width, bytes_accessed=2 * depth * (rows + width), transcendentals=2 * rows * width
    )
    half_cost = pl.CostEstimate(
        flops=rows * depth * width, bytes_accessed=depth * (rows + width), transcendentals=0
    )
    swap = [(i, i ^ 1) for i in range(vocab)]
    mine = pl.pallas_call(
        half_kernel,
        out_shape=jax.ShapeDtypeStruct((rows, half), hidden.dtype),
        in_specs=[pl.BlockSpec(memory_space=pltpu.HBM)],
        out_specs=VMEM,
        scratch_shapes=[pltpu.SemaphoreType.DMA],
        compiler_params=params,
        name="own_half",
    )(hidden)
    near = [lax.ppermute(mine, "dp", [(i, (i + k) % dp) for i in range(dp)]) for k in range(1, dp)]
    tokens = drafts.T
    parts = pl.pallas_call(
        own_kernel,
        out_shape=jax.ShapeDtypeStruct((dp, lines, LANES), jnp.float32),
        in_specs=[VMEM] * 3,
        out_specs=VMEM,
        cost_estimate=cost,
        compiler_params=params,
        name="own_rows",
    )(hidden, head_weight, tokens)
    near, parts = lax.optimization_barrier((near, parts))
    far = [lax.ppermute(block, "vocab", swap) for block in near]
    for k in range(1, dp):
        count = dp * vocab if k == dp - 1 else dp
        logits = pl.pallas_call(
            near_kernel,
            out_shape=jax.ShapeDtypeStruct((rows, width), jnp.float32),
            in_specs=[VMEM] * 2,
            out_specs=VMEM,
            cost_estimate=half_cost,
            compiler_params=params,
            name="near_half",
        )(near[k - 1], head_weight)
        parts = pl.pallas_call(
            functools.partial(far_kernel, k),
            out_shape=jax.ShapeDtypeStruct((count, lines, LANES), jnp.float32),
            in_specs=[VMEM] * 5,
            out_specs=VMEM,
            cost_estimate=half_cost,
            compiler_params=params,
            name="far_half",
        )(far[k - 1], head_weight, logits, tokens, parts)
    parts = lax.all_to_all(parts, ("dp", "vocab"), 0, 0)
    log_norm, logprob, expected, loss = pl.pallas_call(
        functools.partial(tail_kernel, seqs),
        out_shape=(
            jax.ShapeDtypeStruct((POSITIONS, own_seqs), jnp.float32),
            jax.ShapeDtypeStruct((DRAFTS, own_seqs), jnp.float32),
            jax.ShapeDtypeStruct((1, own_seqs), jnp.float32),
            jax.ShapeDtypeStruct((1, 1), jnp.float32),
        ),
        in_specs=[VMEM] * 2,
        out_specs=(VMEM,) * 4,
        compiler_params=params,
        name="tail",
    )(parts, cutoffs.T)
    return log_norm.T, logprob.T, expected.reshape(own_seqs), loss.reshape(())


def solution(mesh):
    in_specs = (P("dp", None), P(None, ("dp", "vocab")), P(), P("dp", None))
    out_specs = (P("dp", None), P("dp", None), P("dp"), P())
    return jax.shard_map(local, mesh=mesh, in_specs=in_specs, out_specs=out_specs, check_vma=False)
```

```python
import functools

import jax
import jax.numpy as jnp
from jax import lax
from jax.experimental import pallas as pl
from jax.experimental.pallas import tpu as pltpu
from jax.sharding import PartitionSpec as P


DRAFTS = 4
POSITIONS = 5
SOFT_CAP = 30.0
Z_WEIGHT = 0.001
LANES = 128
GRANT = 16 * 2**20
RELAYED = 3 * LANES
CHUNKS = 9
VMEM = pl.BlockSpec(memory_space=pltpu.VMEM)


def row_ids(drafts, rows, first_seq):
    shape = (rows, drafts.shape[1])
    seq = lax.broadcasted_iota(jnp.int32, shape, 1) - first_seq
    target = lax.broadcasted_iota(jnp.int32, shape, 0) - seq * POSITIONS
    shifted = (drafts + 1).astype(jnp.float32)
    picked = jnp.zeros(shape, jnp.float32)
    for p in range(DRAFTS):
        picked = jnp.where(target == p, shifted[p : p + 1], picked)
    return jnp.sum(picked, axis=1, keepdims=True).astype(jnp.int32) - 1


def spread(column, starts, lines):
    shape = (column.shape[0], LANES)
    offset = lax.broadcasted_iota(jnp.int32, shape, 0) - POSITIONS * lax.broadcasted_iota(jnp.int32, shape, 1)
    out = []
    for line in range(lines):
        values = jnp.zeros(shape, jnp.float32)
        for p, start in enumerate(starts):
            values = jnp.where(offset == POSITIONS * (line * LANES - start) + p, column, values)
        out.append(jnp.sum(values, axis=0, keepdims=True))
    return jnp.concatenate(out, axis=0)


def payload_lines(seqs, own_seqs):
    return -(-(POSITIONS * seqs + DRAFTS * own_seqs) // LANES)


def contribution(logits, drafts, source):
    rows, width = logits.shape
    seqs, own_seqs = drafts.shape[1], rows // POSITIONS
    shard = lax.axis_index("dp") * lax.axis_size("vocab") + lax.axis_index("vocab")
    ids = row_ids(drafts, rows, source * own_seqs) - shard * width
    capped = SOFT_CAP * jnp.tanh(logits * (1.0 / SOFT_CAP))
    totals = jnp.sum(jnp.exp(capped), axis=1, keepdims=True)
    columns = lax.broadcasted_iota(jnp.int32, (rows, width), 1)
    picks = jnp.sum(jnp.where(columns == ids, capped, 0.0), axis=1, keepdims=True)
    lines = payload_lines(seqs, own_seqs)
    totals = spread(totals, [p * seqs + source * own_seqs for p in range(POSITIONS)], lines)
    picks = spread(picks, [POSITIONS * seqs + p * own_seqs for p in range(DRAFTS)], lines)
    return totals, picks


def parts_for(receiver, source, totals, picks):
    return totals + jnp.where(source == receiver, picks, 0.0)


def place(size, piece, other_row, other_core):
    me = lax.axis_index("vocab")
    core = lax.rem(me + other_core, 2)
    row = lax.rem(me // 2 + other_row, 2)
    return pl.multiple_of((4 * RELAYED + core * size) if piece else (2 * row + core) * size, LANES)


def pieces_kernel(hidden_ref, *piece_refs):
    for piece, ref in enumerate(piece_refs):
        size = ref.shape[1]
        ref[...] = hidden_ref[:, pl.ds(place(size, piece, 0, 0), size)]


def product(rows_ref, weight_ref, piece, other_row, other_core):
    size = rows_ref.shape[1]
    block = weight_ref[pl.ds(place(size, piece, other_row, other_core), size), :]
    return jnp.dot(rows_ref[...], block, preferred_element_type=jnp.float32)


def own_kernel(hidden_ref, weight_ref, drafts_ref, parts_ref, held_ref, tokens_ref, arrived, drafts_arrived):
    depth = weight_ref.shape[0]
    step = depth // CHUNKS
    blocks = [pl.ds(i * step, step) for i in range(CHUNKS)]
    copies = [pltpu.make_async_copy(weight_ref.at[b], held_ref.at[b], arrived.at[i]) for i, b in enumerate(blocks)]
    tokens = pltpu.make_async_copy(drafts_ref, tokens_ref, drafts_arrived)
    for copy in copies:
        copy.start()
    tokens.start()
    logits = jnp.zeros((hidden_ref.shape[0], weight_ref.shape[1]), jnp.float32)
    for block, copy in zip(blocks, copies):
        copy.wait()
        logits += jnp.dot(hidden_ref[:, block], held_ref[block, :], preferred_element_type=jnp.float32)
    tokens.wait()
    me = lax.axis_index("dp")
    totals, picks = contribution(logits, tokens_ref[...], me)
    for receiver in range(parts_ref.shape[0]):
        parts_ref[receiver] = parts_for(receiver, me, totals, picks)


def near_kernel(first_ref, swapped_ref, relayed_ref, second_ref, weight_ref, logits_ref):
    logits = product(first_ref, weight_ref, 0, 0, 0) + product(swapped_ref, weight_ref, 0, 0, 1)
    logits += product(relayed_ref, weight_ref, 0, 1, 0)
    logits_ref[...] = logits + product(second_ref, weight_ref, 1, 0, 0)


def far_kernel(shift, relayed_ref, second_ref, weight_ref, logits_ref, drafts_ref, before_ref, parts_ref):
    dp = before_ref.shape[0]
    copies = parts_ref.shape[0] // dp
    source = lax.rem(lax.axis_index("dp") + dp - shift, dp)
    logits = logits_ref[...] + product(relayed_ref, weight_ref, 0, 1, 1) + product(second_ref, weight_ref, 1, 0, 1)
    totals, picks = contribution(logits, drafts_ref[...], source)
    for receiver in range(dp):
        part = before_ref[receiver] + parts_for(receiver, source, totals, picks)
        parts_ref[receiver * copies : (receiver + 1) * copies] = jnp.broadcast_to(part[None], (copies,) + part.shape)


def gather_rows(flat, starts, count):
    lines = flat.shape[0]
    lane = lax.broadcasted_iota(jnp.int32, (1, LANES), 1)
    out = []
    for low, high, start in starts:
        row = jnp.zeros((1, LANES), jnp.float32)
        for line in range(low // LANES, min(lines, (high - 1) // LANES + 1)):
            place = start - line * LANES
            moved = pltpu.roll(flat, lax.rem(lines * LANES - place, LANES), 1)[line : line + 1]
            row = jnp.where((lane + place >= 0) & (lane + place < LANES), moved, row)
        out.append(row[:, :count])
    return jnp.concatenate(out, axis=0)


def tail_kernel(seqs, parts_ref, cutoffs_ref, norm_ref, logprob_ref, expected_ref, loss_ref):
    own_seqs = cutoffs_ref.shape[1]
    flat = jnp.sum(parts_ref[...], axis=0)
    place = lax.broadcasted_iota(jnp.int32, flat.shape, 0) * LANES + lax.broadcasted_iota(jnp.int32, flat.shape, 1)
    log_total = jnp.log(jnp.where(place < POSITIONS * seqs, flat, 1.0))
    squares = jnp.sum(jnp.sum(log_total * log_total, axis=1, keepdims=True), axis=0, keepdims=True)
    loss_ref[...] = squares * (Z_WEIGHT / (seqs * POSITIONS))
    first = lax.axis_index("dp") * own_seqs
    ranges = [(p * seqs, (p + 1) * seqs, p * seqs + first) for p in range(POSITIONS)]
    log_norm = gather_rows(log_total, ranges, own_seqs)
    base = POSITIONS * seqs
    ranges = [(base + p * own_seqs, base + (p + 1) * own_seqs, base + p * own_seqs) for p in range(DRAFTS)]
    picks = gather_rows(flat, ranges, own_seqs)
    norm_ref[...] = log_norm
    logprob = picks - log_norm[:DRAFTS]
    logprob_ref[...] = logprob
    accept = jax.nn.sigmoid(logprob - cutoffs_ref[...].astype(jnp.float32) / 1024.0)
    product = accept[0:1]
    expected = product
    for p in range(1, DRAFTS):
        product = product * accept[p : p + 1]
        expected = expected + product
    expected_ref[...] = expected


def local(hidden, head_weight, drafts, cutoffs):
    dp, vocab = lax.axis_size("dp"), lax.axis_size("vocab")
    rows, depth = hidden.shape
    width = head_weight.shape[1]
    seqs, own_seqs = drafts.shape[0], rows // POSITIONS
    second = depth // 2 - 2 * RELAYED
    lines = payload_lines(seqs, own_seqs)
    params = pltpu.CompilerParams(vmem_limit_bytes=GRANT)
    cost = pl.CostEstimate(
        flops=2 * rows * depth * width, bytes_accessed=2 * depth * (rows + width), transcendentals=2 * rows * width
    )
    half_cost = pl.CostEstimate(
        flops=rows * depth * width, bytes_accessed=depth * (rows + width), transcendentals=0
    )
    swap = [(i, i ^ 1) for i in range(vocab)]
    relay = [(i, i ^ 2) for i in range(vocab)]
    pieces = pl.pallas_call(
        pieces_kernel,
        out_shape=[jax.ShapeDtypeStruct((rows, size), hidden.dtype) for size in (RELAYED, second)],
        in_specs=[VMEM],
        out_specs=[VMEM] * 2,
        compiler_params=params,
        name="pieces",
    )(hidden)
    others = []
    for k in range(1, dp):
        shift = [(i, (i + k) % dp) for i in range(dp)]
        first = lax.ppermute(pieces[0], "dp", shift)
        both = lax.ppermute(pieces[1], "dp", shift)
        relayed = lax.ppermute(first, "vocab", relay)
        others.append((first, both, relayed, lax.ppermute(first, "vocab", swap)))
    parts, held, tokens = pl.pallas_call(
        own_kernel,
        out_shape=(
            jax.ShapeDtypeStruct((dp, lines, LANES), jnp.float32),
            pltpu.VMEM(head_weight.shape, head_weight.dtype),
            pltpu.VMEM((DRAFTS, seqs), drafts.dtype),
        ),
        in_specs=[VMEM, pl.BlockSpec(memory_space=pl.ANY), pl.BlockSpec(memory_space=pl.ANY)],
        out_specs=(VMEM,) * 3,
        scratch_shapes=[pltpu.SemaphoreType.DMA((CHUNKS,)), pltpu.SemaphoreType.DMA],
        cost_estimate=cost,
        compiler_params=params,
        name="own_rows",
    )(
        hidden,
        pltpu.with_memory_space_constraint(head_weight, pltpu.HBM),
        pltpu.with_memory_space_constraint(drafts.T, pltpu.HBM),
    )
    for k in range(1, dp):
        first, both, relayed, first_swapped = others[k - 1]
        both, relayed, first_swapped = lax.optimization_barrier((both, relayed, first_swapped))
        relayed_swapped = lax.ppermute(relayed, "vocab", swap)
        both_swapped = lax.ppermute(both, "vocab", swap)
        count = dp * vocab if k == dp - 1 else dp
        logits = pl.pallas_call(
            near_kernel,
            out_shape=jax.ShapeDtypeStruct((rows, width), jnp.float32),
            in_specs=[VMEM] * 5,
            out_specs=VMEM,
            cost_estimate=half_cost,
            compiler_params=params,
            name="near",
        )(first, first_swapped, relayed, both, held)
        parts = pl.pallas_call(
            functools.partial(far_kernel, k),
            out_shape=jax.ShapeDtypeStruct((count, lines, LANES), jnp.float32),
            in_specs=[VMEM] * 6,
            out_specs=VMEM,
            cost_estimate=half_cost,
            compiler_params=params,
            name="far",
        )(relayed_swapped, both_swapped, held, logits, tokens, parts)
    parts = lax.all_to_all(parts, ("dp", "vocab"), 0, 0)
    log_norm, logprob, expected, loss = pl.pallas_call(
        functools.partial(tail_kernel, seqs),
        out_shape=(
            jax.ShapeDtypeStruct((POSITIONS, own_seqs), jnp.float32),
            jax.ShapeDtypeStruct((DRAFTS, own_seqs), jnp.float32),
            jax.ShapeDtypeStruct((1, own_seqs), jnp.float32),
            jax.ShapeDtypeStruct((1, 1), jnp.float32),
        ),
        in_specs=[VMEM] * 2,
        out_specs=(VMEM,) * 4,
        compiler_params=params,
        name="tail",
    )(parts, cutoffs.T)
    return log_norm.T, logprob.T, expected.reshape(own_seqs), loss.reshape(())


def solution(mesh):
    in_specs = (P("dp", None), P(None, ("dp", "vocab")), P(), P("dp", None))
    out_specs = (P("dp", None), P("dp", None), P("dp"), P())
    return jax.shard_map(local, mesh=mesh, in_specs=in_specs, out_specs=out_specs, check_vma=False)
```

```python
import functools

import jax
import jax.numpy as jnp
from jax import lax
from jax.experimental import pallas as pl
from jax.experimental.pallas import tpu as pltpu
from jax.sharding import PartitionSpec as P


DRAFTS = 4
POSITIONS = 5
SOFT_CAP = 30.0
Z_WEIGHT = 0.001
LANES = 128
GRANT = 16 * 2**20
RELAYED = 3 * LANES
EARLY = 8 * LANES
WEIGHT_HINT = 3_000_000_000
VMEM = pl.BlockSpec(memory_space=pltpu.VMEM)
ANY = pl.BlockSpec(memory_space=pl.ANY)


def row_ids(drafts, rows, first_seq):
    shape = (rows, drafts.shape[1])
    seq = lax.broadcasted_iota(jnp.int32, shape, 1) - first_seq
    target = lax.broadcasted_iota(jnp.int32, shape, 0) - seq * POSITIONS
    shifted = (drafts + 1).astype(jnp.float32)
    picked = jnp.zeros(shape, jnp.float32)
    for p in range(DRAFTS):
        picked = jnp.where(target == p, shifted[p : p + 1], picked)
    return jnp.sum(picked, axis=1, keepdims=True).astype(jnp.int32) - 1


def spread(column, starts, lines):
    shape = (column.shape[0], LANES)
    offset = lax.broadcasted_iota(jnp.int32, shape, 0) - POSITIONS * lax.broadcasted_iota(jnp.int32, shape, 1)
    out = []
    for line in range(lines):
        values = jnp.zeros(shape, jnp.float32)
        for p, start in enumerate(starts):
            values = jnp.where(offset == POSITIONS * (line * LANES - start) + p, column, values)
        out.append(jnp.sum(values, axis=0, keepdims=True))
    return jnp.concatenate(out, axis=0)


def payload_lines(seqs, own_seqs):
    return -(-(POSITIONS * seqs + DRAFTS * own_seqs) // LANES)


def contribution(logits, drafts, source):
    rows, width = logits.shape
    seqs, own_seqs = drafts.shape[1], rows // POSITIONS
    shard = lax.axis_index("dp") * lax.axis_size("vocab") + lax.axis_index("vocab")
    ids = row_ids(drafts, rows, source * own_seqs) - shard * width
    capped = SOFT_CAP * jnp.tanh(logits * (1.0 / SOFT_CAP))
    totals = jnp.sum(jnp.exp(capped), axis=1, keepdims=True)
    columns = lax.broadcasted_iota(jnp.int32, (rows, width), 1)
    picks = jnp.sum(jnp.where(columns == ids, capped, 0.0), axis=1, keepdims=True)
    lines = payload_lines(seqs, own_seqs)
    totals = spread(totals, [p * seqs + source * own_seqs for p in range(POSITIONS)], lines)
    picks = spread(picks, [POSITIONS * seqs + p * own_seqs for p in range(DRAFTS)], lines)
    return totals, picks


def parts_for(receiver, source, totals, picks):
    return totals + jnp.where(source == receiver, picks, 0.0)


def place(size, piece, other_row, other_core):
    me = lax.axis_index("vocab")
    core = lax.rem(me + other_core, 2)
    row = lax.rem(me // 2 + other_row, 2)
    base = (2 * row * RELAYED, 4 * RELAYED, 4 * RELAYED + 2 * EARLY)[piece]
    return pl.multiple_of(base + core * size, LANES)


def pieces_kernel(hidden_ref, *piece_refs):
    for piece, ref in enumerate(piece_refs):
        size = ref.shape[1]
        ref[...] = hidden_ref[:, pl.ds(place(size, piece, 0, 0), size)]


def product(rows_ref, weight_ref, piece, other_row, other_core):
    size = rows_ref.shape[1]
    block = weight_ref[pl.ds(place(size, piece, other_row, other_core), size), :]
    return jnp.dot(rows_ref[...], block, preferred_element_type=jnp.float32)


def tokens_kernel(drafts_ref, tokens_ref, arrived):
    copy = pltpu.make_async_copy(drafts_ref, tokens_ref, arrived)
    copy.start()
    copy.wait()


def own_kernel(hidden_ref, weight_ref, tokens_ref, parts_ref):
    logits = jnp.dot(hidden_ref[...], weight_ref[...], preferred_element_type=jnp.float32)
    me = lax.axis_index("dp")
    totals, picks = contribution(logits, tokens_ref[...], me)
    for receiver in range(parts_ref.shape[0]):
        parts_ref[receiver] = parts_for(receiver, me, totals, picks)


def near_kernel(first_ref, swapped_ref, early_ref, weight_ref, logits_ref):
    logits = product(first_ref, weight_ref, 0, 0, 0) + product(swapped_ref, weight_ref, 0, 0, 1)
    logits_ref[...] = logits + product(early_ref, weight_ref, 1, 0, 0)


def middle_kernel(swapped_ref, relayed_ref, late_ref, weight_ref, before_ref, logits_ref):
    logits = before_ref[...] + product(swapped_ref, weight_ref, 1, 0, 1)
    logits += product(relayed_ref, weight_ref, 0, 1, 0)
    logits_ref[...] = logits + product(late_ref, weight_ref, 2, 0, 0)


def far_kernel(shift, relayed_ref, late_ref, weight_ref, logits_ref, drafts_ref, before_ref, parts_ref):
    dp = before_ref.shape[0]
    copies = parts_ref.shape[0] // dp
    source = lax.rem(lax.axis_index("dp") + dp - shift, dp)
    logits = logits_ref[...] + product(relayed_ref, weight_ref, 0, 1, 1) + product(late_ref, weight_ref, 2, 0, 1)
    totals, picks = contribution(logits, drafts_ref[...], source)
    for receiver in range(dp):
        part = before_ref[receiver] + parts_for(receiver, source, totals, picks)
        parts_ref[receiver * copies : (receiver + 1) * copies] = jnp.broadcast_to(part[None], (copies,) + part.shape)


def gather_rows(flat, starts, count):
    lines = flat.shape[0]
    lane = lax.broadcasted_iota(jnp.int32, (1, LANES), 1)
    out = []
    for low, high, start in starts:
        row = jnp.zeros((1, LANES), jnp.float32)
        for line in range(low // LANES, min(lines, (high - 1) // LANES + 1)):
            place = start - line * LANES
            moved = pltpu.roll(flat, lax.rem(lines * LANES - place, LANES), 1)[line : line + 1]
            row = jnp.where((lane + place >= 0) & (lane + place < LANES), moved, row)
        out.append(row[:, :count])
    return jnp.concatenate(out, axis=0)


def tail_kernel(seqs, parts_ref, cutoffs_ref, norm_ref, logprob_ref, expected_ref, loss_ref):
    own_seqs = cutoffs_ref.shape[1]
    flat = jnp.sum(parts_ref[...], axis=0)
    place = lax.broadcasted_iota(jnp.int32, flat.shape, 0) * LANES + lax.broadcasted_iota(jnp.int32, flat.shape, 1)
    log_total = jnp.log(jnp.where(place < POSITIONS * seqs, flat, 1.0))
    squares = jnp.sum(jnp.sum(log_total * log_total, axis=1, keepdims=True), axis=0, keepdims=True)
    loss_ref[...] = squares * (Z_WEIGHT / (seqs * POSITIONS))
    first = lax.axis_index("dp") * own_seqs
    ranges = [(p * seqs, (p + 1) * seqs, p * seqs + first) for p in range(POSITIONS)]
    log_norm = gather_rows(log_total, ranges, own_seqs)
    base = POSITIONS * seqs
    ranges = [(base + p * own_seqs, base + (p + 1) * own_seqs, base + p * own_seqs) for p in range(DRAFTS)]
    picks = gather_rows(flat, ranges, own_seqs)
    norm_ref[...] = log_norm
    logprob = picks - log_norm[:DRAFTS]
    logprob_ref[...] = logprob
    accept = jax.nn.sigmoid(logprob - cutoffs_ref[...].astype(jnp.float32) / 1024.0)
    product = accept[0:1]
    expected = product
    for p in range(1, DRAFTS):
        product = product * accept[p : p + 1]
        expected = expected + product
    expected_ref[...] = expected


def local(hidden, head_weight, drafts, cutoffs):
    dp, vocab = lax.axis_size("dp"), lax.axis_size("vocab")
    rows, depth = hidden.shape
    width = head_weight.shape[1]
    seqs, own_seqs = drafts.shape[0], rows // POSITIONS
    late_size = depth // 2 - 2 * RELAYED - EARLY
    lines = payload_lines(seqs, own_seqs)
    params = pltpu.CompilerParams(vmem_limit_bytes=GRANT)
    cost = pl.CostEstimate(
        flops=2 * rows * depth * width, bytes_accessed=2 * depth * (rows + width), transcendentals=2 * rows * width
    )
    third_cost = pl.CostEstimate(
        flops=rows * depth * width // 2, bytes_accessed=depth * (rows + width) // 2, transcendentals=0
    )
    swap = [(i, i ^ 1) for i in range(vocab)]
    relay = [(i, i ^ 2) for i in range(vocab)]
    first_piece, early_piece, late_piece = pl.pallas_call(
        pieces_kernel,
        out_shape=[jax.ShapeDtypeStruct((rows, size), hidden.dtype) for size in (RELAYED, EARLY, late_size)],
        in_specs=[VMEM],
        out_specs=[VMEM] * 3,
        compiler_params=params,
        name="pieces",
    )(hidden)
    logits_shape = jax.ShapeDtypeStruct((rows, width), jnp.float32)
    for k in range(1, dp):
        shift = [(i, (i + k) % dp) for i in range(dp)]
        first = lax.ppermute(first_piece, "dp", shift)
        early = lax.ppermute(early_piece, "dp", shift)
        late = lax.ppermute(late_piece, "dp", shift)
        relayed = lax.ppermute(first, "vocab", relay)
        first_swapped = lax.ppermute(first, "vocab", swap)
        if k == 1:
            tokens = pl.pallas_call(
                tokens_kernel,
                out_shape=pltpu.VMEM((DRAFTS, seqs), drafts.dtype),
                in_specs=[pl.BlockSpec(memory_space=pl.ANY)],
                out_specs=VMEM,
                scratch_shapes=[pltpu.SemaphoreType.DMA],
                cost_estimate=pl.CostEstimate(flops=WEIGHT_HINT, bytes_accessed=0, transcendentals=0),
                compiler_params=params,
                name="tokens",
            )(pltpu.with_memory_space_constraint(drafts.T, pltpu.HBM))
            parts = pl.pallas_call(
                own_kernel,
                out_shape=jax.ShapeDtypeStruct((dp, lines, LANES), jnp.float32),
                in_specs=[VMEM] * 3,
                out_specs=VMEM,
                cost_estimate=cost,
                compiler_params=params,
                name="own_rows",
            )(hidden, head_weight, tokens)
        early, first_swapped = lax.optimization_barrier((early, first_swapped))
        early_swapped = lax.ppermute(early, "vocab", swap)
        logits = pl.pallas_call(
            near_kernel,
            out_shape=logits_shape,
            in_specs=[VMEM] * 4,
            out_specs=VMEM,
            cost_estimate=third_cost,
            compiler_params=params,
            name="near",
        )(first, first_swapped, early, head_weight)
        late, relayed, logits = lax.optimization_barrier((late, relayed, logits))
        relayed_swapped = lax.ppermute(relayed, "vocab", swap)
        late_swapped = lax.ppermute(late, "vocab", swap)
        logits = pl.pallas_call(
            middle_kernel,
            out_shape=logits_shape,
            in_specs=[VMEM] * 5,
            out_specs=VMEM,
            cost_estimate=third_cost,
            compiler_params=params,
            name="middle",
        )(early_swapped, relayed, late, head_weight, logits)
        count = dp * vocab if k == dp - 1 else dp
        parts = pl.pallas_call(
            functools.partial(far_kernel, k),
            out_shape=jax.ShapeDtypeStruct((count, lines, LANES), jnp.float32),
            in_specs=[VMEM] * 6,
            out_specs=VMEM,
            cost_estimate=third_cost,
            compiler_params=params,
            name="far",
        )(relayed_swapped, late_swapped, head_weight, logits, tokens, parts)
        if k < dp - 1:
            pieces = first_piece, early_piece, late_piece
            (first_piece, early_piece, late_piece), parts = lax.optimization_barrier((pieces, parts))
    parts = lax.all_to_all(parts, ("dp", "vocab"), 0, 0)
    log_norm, logprob, expected, loss = pl.pallas_call(
        functools.partial(tail_kernel, seqs),
        out_shape=(
            jax.ShapeDtypeStruct((POSITIONS, own_seqs), jnp.float32),
            jax.ShapeDtypeStruct((DRAFTS, own_seqs), jnp.float32),
            jax.ShapeDtypeStruct((1, own_seqs), jnp.float32),
            jax.ShapeDtypeStruct((1, 1), jnp.float32),
        ),
        in_specs=[VMEM] * 2,
        out_specs=(VMEM,) * 4,
        compiler_params=params,
        name="tail",
    )(parts, cutoffs.T)
    return log_norm.T, logprob.T, expected.reshape(own_seqs), loss.reshape(())


def solution(mesh):
    in_specs = (P("dp", None), P(None, ("dp", "vocab")), P(), P("dp", None))
    out_specs = (P("dp", None), P("dp", None), P("dp"), P())
    return jax.shard_map(local, mesh=mesh, in_specs=in_specs, out_specs=out_specs, check_vma=False)
```

```python
import functools

import jax
import jax.numpy as jnp
from jax import lax
from jax.experimental import pallas as pl
from jax.experimental.pallas import tpu as pltpu
from jax.sharding import PartitionSpec as P


DRAFTS = 4
POSITIONS = 5
SOFT_CAP = 30.0
Z_WEIGHT = 0.001
LANES = 128
SUBLANES = 8
GRANT = 16 * 2**20
RELAYED = 3 * LANES
EARLY = 8 * LANES
HIDDEN_HINT = 1_200_000_000
WEIGHT_HINT = 3_000_000_000
VMEM = pl.BlockSpec(memory_space=pltpu.VMEM)
ANY = pl.BlockSpec(memory_space=pl.ANY)


def row_ids(drafts, rows, first_seq):
    shape = (rows, drafts.shape[1])
    seq = lax.broadcasted_iota(jnp.int32, shape, 1) - first_seq
    target = lax.broadcasted_iota(jnp.int32, shape, 0) - seq * POSITIONS
    shifted = (drafts + 1).astype(jnp.float32)
    picked = jnp.zeros(shape, jnp.float32)
    for p in range(DRAFTS):
        picked = jnp.where(target == p, shifted[p : p + 1], picked)
    return jnp.sum(picked, axis=1, keepdims=True).astype(jnp.int32) - 1


def spread(column, starts, lines):
    shape = (column.shape[0], LANES)
    offset = lax.broadcasted_iota(jnp.int32, shape, 0) - POSITIONS * lax.broadcasted_iota(jnp.int32, shape, 1)
    out = []
    for line in range(lines):
        values = jnp.zeros(shape, jnp.float32)
        for p, start in enumerate(starts):
            values = jnp.where(offset == POSITIONS * (line * LANES - start) + p, column, values)
        out.append(jnp.sum(values, axis=0, keepdims=True))
    return jnp.concatenate(out, axis=0)


def payload_lines(seqs, own_seqs):
    return -(-(POSITIONS * seqs + DRAFTS * own_seqs) // LANES)


def contribution(logits, drafts, source):
    rows, width = logits.shape
    seqs, own_seqs = drafts.shape[1], rows // POSITIONS
    shard = lax.axis_index("dp") * lax.axis_size("vocab") + lax.axis_index("vocab")
    ids = row_ids(drafts, rows, source * own_seqs) - shard * width
    capped = SOFT_CAP * jnp.tanh(logits * (1.0 / SOFT_CAP))
    totals = jnp.sum(jnp.exp(capped), axis=1, keepdims=True)
    columns = lax.broadcasted_iota(jnp.int32, (rows, width), 1)
    picks = jnp.sum(jnp.where(columns == ids, capped, 0.0), axis=1, keepdims=True)
    lines = payload_lines(seqs, own_seqs)
    totals = spread(totals, [p * seqs + source * own_seqs for p in range(POSITIONS)], lines)
    picks = spread(picks, [POSITIONS * seqs + p * own_seqs for p in range(DRAFTS)], lines)
    return totals, picks


def parts_for(receiver, source, totals, picks):
    return totals + jnp.where(source == receiver, picks, 0.0)


def place(size, piece, other_row, other_core):
    me = lax.axis_index("vocab")
    core = lax.rem(me + other_core, 2)
    row = lax.rem(me // 2 + other_row, 2)
    base = (2 * row * RELAYED, 4 * RELAYED, 4 * RELAYED + 2 * EARLY)[piece]
    return pl.multiple_of(base + core * size, LANES)


def first_kernel(hidden_ref, piece_ref, arrived):
    rows, size = piece_ref.shape
    columns = pl.ds(place(size, 0, 0, 0), size)
    groups = [pl.ds(i, SUBLANES) for i in range(0, rows, SUBLANES)]
    copies = [
        pltpu.make_async_copy(hidden_ref.at[g, columns], piece_ref.at[g], arrived.at[i]) for i, g in enumerate(groups)
    ]
    for copy in copies:
        copy.start()
    for copy in copies:
        copy.wait()


def pieces_kernel(hidden_ref, *piece_refs):
    for piece, ref in enumerate(piece_refs, 1):
        size = ref.shape[1]
        ref[...] = hidden_ref[:, pl.ds(place(size, piece, 0, 0), size)]


def product(rows_ref, weight_ref, piece, other_row, other_core):
    size = rows_ref.shape[1]
    block = weight_ref[pl.ds(place(size, piece, other_row, other_core), size), :]
    return jnp.dot(rows_ref[...], block, preferred_element_type=jnp.float32)


def tokens_kernel(drafts_ref, tokens_ref, arrived):
    copy = pltpu.make_async_copy(drafts_ref, tokens_ref, arrived)
    copy.start()
    copy.wait()


def own_kernel(hidden_ref, weight_ref, tokens_ref, parts_ref):
    logits = jnp.dot(hidden_ref[...], weight_ref[...], preferred_element_type=jnp.float32)
    me = lax.axis_index("dp")
    totals, picks = contribution(logits, tokens_ref[...], me)
    for receiver in range(parts_ref.shape[0]):
        parts_ref[receiver] = parts_for(receiver, me, totals, picks)


def near_kernel(first_ref, swapped_ref, early_ref, weight_ref, logits_ref):
    logits = product(first_ref, weight_ref, 0, 0, 0) + product(swapped_ref, weight_ref, 0, 0, 1)
    logits_ref[...] = logits + product(early_ref, weight_ref, 1, 0, 0)


def middle_kernel(swapped_ref, relayed_ref, late_ref, weight_ref, before_ref, logits_ref):
    logits = before_ref[...] + product(swapped_ref, weight_ref, 1, 0, 1)
    logits += product(relayed_ref, weight_ref, 0, 1, 0)
    logits_ref[...] = logits + product(late_ref, weight_ref, 2, 0, 0)


def far_kernel(shift, relayed_ref, late_ref, weight_ref, logits_ref, drafts_ref, before_ref, parts_ref):
    dp = before_ref.shape[0]
    copies = parts_ref.shape[0] // dp
    source = lax.rem(lax.axis_index("dp") + dp - shift, dp)
    logits = logits_ref[...] + product(relayed_ref, weight_ref, 0, 1, 1) + product(late_ref, weight_ref, 2, 0, 1)
    totals, picks = contribution(logits, drafts_ref[...], source)
    for receiver in range(dp):
        part = before_ref[receiver] + parts_for(receiver, source, totals, picks)
        parts_ref[receiver * copies : (receiver + 1) * copies] = jnp.broadcast_to(part[None], (copies,) + part.shape)


def gather_rows(flat, starts, count):
    lines = flat.shape[0]
    lane = lax.broadcasted_iota(jnp.int32, (1, LANES), 1)
    out = []
    for low, high, start in starts:
        row = jnp.zeros((1, LANES), jnp.float32)
        for line in range(low // LANES, min(lines, (high - 1) // LANES + 1)):
            place = start - line * LANES
            moved = pltpu.roll(flat, lax.rem(lines * LANES - place, LANES), 1)[line : line + 1]
            row = jnp.where((lane + place >= 0) & (lane + place < LANES), moved, row)
        out.append(row[:, :count])
    return jnp.concatenate(out, axis=0)


def tail_kernel(seqs, parts_ref, cutoffs_ref, norm_ref, logprob_ref, expected_ref, loss_ref):
    own_seqs = cutoffs_ref.shape[1]
    flat = jnp.sum(parts_ref[...], axis=0)
    place = lax.broadcasted_iota(jnp.int32, flat.shape, 0) * LANES + lax.broadcasted_iota(jnp.int32, flat.shape, 1)
    log_total = jnp.log(jnp.where(place < POSITIONS * seqs, flat, 1.0))
    squares = jnp.sum(jnp.sum(log_total * log_total, axis=1, keepdims=True), axis=0, keepdims=True)
    loss_ref[...] = squares * (Z_WEIGHT / (seqs * POSITIONS))
    first = lax.axis_index("dp") * own_seqs
    ranges = [(p * seqs, (p + 1) * seqs, p * seqs + first) for p in range(POSITIONS)]
    log_norm = gather_rows(log_total, ranges, own_seqs)
    base = POSITIONS * seqs
    ranges = [(base + p * own_seqs, base + (p + 1) * own_seqs, base + p * own_seqs) for p in range(DRAFTS)]
    picks = gather_rows(flat, ranges, own_seqs)
    norm_ref[...] = log_norm
    logprob = picks - log_norm[:DRAFTS]
    logprob_ref[...] = logprob
    accept = jax.nn.sigmoid(logprob - cutoffs_ref[...].astype(jnp.float32) / 1024.0)
    product = accept[0:1]
    expected = product
    for p in range(1, DRAFTS):
        product = product * accept[p : p + 1]
        expected = expected + product
    expected_ref[...] = expected


def local(hidden, head_weight, drafts, cutoffs):
    dp, vocab = lax.axis_size("dp"), lax.axis_size("vocab")
    rows, depth = hidden.shape
    width = head_weight.shape[1]
    seqs, own_seqs = drafts.shape[0], rows // POSITIONS
    late_size = depth // 2 - 2 * RELAYED - EARLY
    lines = payload_lines(seqs, own_seqs)
    params = pltpu.CompilerParams(vmem_limit_bytes=GRANT)
    cost = pl.CostEstimate(
        flops=2 * rows * depth * width, bytes_accessed=2 * depth * (rows + width), transcendentals=2 * rows * width
    )
    third_cost = pl.CostEstimate(
        flops=rows * depth * width // 2, bytes_accessed=depth * (rows + width) // 2, transcendentals=0
    )
    swap = [(i, i ^ 1) for i in range(vocab)]
    relay = [(i, i ^ 2) for i in range(vocab)]
    first_piece = pl.pallas_call(
        first_kernel,
        out_shape=jax.ShapeDtypeStruct((rows, RELAYED), hidden.dtype),
        in_specs=[pl.BlockSpec(memory_space=pl.ANY)],
        out_specs=VMEM,
        scratch_shapes=[pltpu.SemaphoreType.DMA((rows // SUBLANES,))],
        cost_estimate=pl.CostEstimate(flops=HIDDEN_HINT, bytes_accessed=0, transcendentals=0),
        compiler_params=params,
        name="first_piece",
    )(pltpu.with_memory_space_constraint(hidden, pltpu.HBM))
    early_piece, late_piece = pl.pallas_call(
        pieces_kernel,
        out_shape=[jax.ShapeDtypeStruct((rows, size), hidden.dtype) for size in (EARLY, late_size)],
        in_specs=[VMEM],
        out_specs=[VMEM] * 2,
        compiler_params=params,
        name="pieces",
    )(hidden)
    logits_shape = jax.ShapeDtypeStruct((rows, width), jnp.float32)
    for k in range(1, dp):
        shift = [(i, (i + k) % dp) for i in range(dp)]
        first = lax.ppermute(first_piece, "dp", shift)
        early = lax.ppermute(early_piece, "dp", shift)
        late = lax.ppermute(late_piece, "dp", shift)
        relayed = lax.ppermute(first, "vocab", relay)
        first_swapped = lax.ppermute(first, "vocab", swap)
        if k == 1:
            tokens = pl.pallas_call(
                tokens_kernel,
                out_shape=pltpu.VMEM((DRAFTS, seqs), drafts.dtype),
                in_specs=[pl.BlockSpec(memory_space=pl.ANY)],
                out_specs=VMEM,
                scratch_shapes=[pltpu.SemaphoreType.DMA],
                cost_estimate=pl.CostEstimate(flops=WEIGHT_HINT, bytes_accessed=0, transcendentals=0),
                compiler_params=params,
                name="tokens",
            )(pltpu.with_memory_space_constraint(drafts.T, pltpu.HBM))
            parts = pl.pallas_call(
                own_kernel,
                out_shape=jax.ShapeDtypeStruct((dp, lines, LANES), jnp.float32),
                in_specs=[VMEM] * 3,
                out_specs=VMEM,
                cost_estimate=cost,
                compiler_params=params,
                name="own_rows",
            )(hidden, head_weight, tokens)
        early, first_swapped = lax.optimization_barrier((early, first_swapped))
        early_swapped = lax.ppermute(early, "vocab", swap)
        logits = pl.pallas_call(
            near_kernel,
            out_shape=logits_shape,
            in_specs=[VMEM] * 4,
            out_specs=VMEM,
            cost_estimate=third_cost,
            compiler_params=params,
            name="near",
        )(first, first_swapped, early, head_weight)
        late, relayed, logits = lax.optimization_barrier((late, relayed, logits))
        relayed_swapped = lax.ppermute(relayed, "vocab", swap)
        late_swapped = lax.ppermute(late, "vocab", swap)
        logits = pl.pallas_call(
            middle_kernel,
            out_shape=logits_shape,
            in_specs=[VMEM] * 5,
            out_specs=VMEM,
            cost_estimate=third_cost,
            compiler_params=params,
            name="middle",
        )(early_swapped, relayed, late, head_weight, logits)
        count = dp * vocab if k == dp - 1 else dp
        parts = pl.pallas_call(
            functools.partial(far_kernel, k),
            out_shape=jax.ShapeDtypeStruct((count, lines, LANES), jnp.float32),
            in_specs=[VMEM] * 6,
            out_specs=VMEM,
            cost_estimate=third_cost,
            compiler_params=params,
            name="far",
        )(relayed_swapped, late_swapped, head_weight, logits, tokens, parts)
        if k < dp - 1:
            pieces = first_piece, early_piece, late_piece
            (first_piece, early_piece, late_piece), parts = lax.optimization_barrier((pieces, parts))
    parts = lax.all_to_all(parts, ("dp", "vocab"), 0, 0)
    log_norm, logprob, expected, loss = pl.pallas_call(
        functools.partial(tail_kernel, seqs),
        out_shape=(
            jax.ShapeDtypeStruct((POSITIONS, own_seqs), jnp.float32),
            jax.ShapeDtypeStruct((DRAFTS, own_seqs), jnp.float32),
            jax.ShapeDtypeStruct((1, own_seqs), jnp.float32),
            jax.ShapeDtypeStruct((1, 1), jnp.float32),
        ),
        in_specs=[VMEM] * 2,
        out_specs=(VMEM,) * 4,
        compiler_params=params,
        name="tail",
    )(parts, cutoffs.T)
    return log_norm.T, logprob.T, expected.reshape(own_seqs), loss.reshape(())


def solution(mesh):
    in_specs = (P("dp", None), P(None, ("dp", "vocab")), P(), P("dp", None))
    out_specs = (P("dp", None), P("dp", None), P("dp"), P())
    return jax.shard_map(local, mesh=mesh, in_specs=in_specs, out_specs=out_specs, check_vma=False)
```

```python
import functools

import jax
import jax.numpy as jnp
from jax import lax
from jax.experimental import pallas as pl
from jax.experimental.pallas import tpu as pltpu
from jax.sharding import PartitionSpec as P


DRAFTS = 4
POSITIONS = 5
SOFT_CAP = 30.0
Z_WEIGHT = 0.001
LANES = 128
SUBLANES = 8
GRANT = 16 * 2**20
RELAYED = 6 * LANES
EARLY = 16 * LANES
HIDDEN_HINT = 1_200_000_000
WEIGHT_HINT = 3_000_000_000
VMEM = pl.BlockSpec(memory_space=pltpu.VMEM)
ANY = pl.BlockSpec(memory_space=pl.ANY)


def row_ids(drafts, rows, first_seq):
    shape = (rows, drafts.shape[1])
    seq = lax.broadcasted_iota(jnp.int32, shape, 1) - first_seq
    target = lax.broadcasted_iota(jnp.int32, shape, 0) - seq * POSITIONS
    shifted = (drafts + 1).astype(jnp.float32)
    picked = jnp.zeros(shape, jnp.float32)
    for p in range(DRAFTS):
        picked = jnp.where(target == p, shifted[p : p + 1], picked)
    return jnp.sum(picked, axis=1, keepdims=True).astype(jnp.int32) - 1


def spread(column, starts, lines):
    shape = (column.shape[0], LANES)
    offset = lax.broadcasted_iota(jnp.int32, shape, 0) - POSITIONS * lax.broadcasted_iota(jnp.int32, shape, 1)
    out = []
    for line in range(lines):
        values = jnp.zeros(shape, jnp.float32)
        for p, start in enumerate(starts):
            values = jnp.where(offset == POSITIONS * (line * LANES - start) + p, column, values)
        out.append(jnp.sum(values, axis=0, keepdims=True))
    return jnp.concatenate(out, axis=0)


def payload_lines(seqs, own_seqs):
    return -(-(POSITIONS * seqs + DRAFTS * own_seqs) // LANES)


def contribution(blocks, drafts, own_seqs, first_seq, local_seq):
    rows, width = blocks[0][0].shape
    seqs = drafts.shape[1]
    ids = row_ids(drafts, rows, first_seq)
    columns = lax.broadcasted_iota(jnp.int32, (rows, width), 1)
    totals = picks = 0.0
    for logits, shard in blocks:
        capped = SOFT_CAP * jnp.tanh(logits * (1.0 / SOFT_CAP))
        totals += jnp.exp(capped)
        picks += jnp.where(columns == ids - shard * width, capped, 0.0)
    totals = jnp.sum(totals, axis=1, keepdims=True)
    picks = jnp.sum(picks, axis=1, keepdims=True)
    lines = payload_lines(seqs, own_seqs)
    totals = spread(totals, [p * seqs + first_seq for p in range(POSITIONS)], lines)
    picks = spread(picks, [POSITIONS * seqs + p * own_seqs + local_seq for p in range(DRAFTS)], lines)
    return totals, picks


def parts_for(receiver, source, totals, picks):
    return totals + jnp.where(source == receiver, picks, 0.0)


def place(piece, other_row):
    if piece:
        return 2 * RELAYED + (piece - 1) * EARLY
    row = lax.rem(lax.axis_index("vocab") // 2 + other_row, 2)
    return pl.multiple_of(row * RELAYED, LANES)


def half_start(rows):
    return pl.multiple_of(lax.rem(lax.axis_index("vocab"), 2) * rows, SUBLANES)


def first_kernel(hidden_ref, piece_ref, arrived):
    rows, size = piece_ref.shape
    source = hidden_ref.at[pl.ds(half_start(rows), rows), pl.ds(place(0, 0), size)]
    copy = pltpu.make_async_copy(source, piece_ref, arrived)
    copy.start()
    copy.wait()


def pieces_kernel(hidden_ref, *piece_refs):
    for piece, ref in enumerate(piece_refs, 1):
        rows, size = ref.shape
        ref[...] = hidden_ref[pl.ds(half_start(rows), rows), pl.ds(place(piece, 0), size)]


def product(rows_ref, weight_refs, piece, other_row):
    block = pl.ds(place(piece, other_row), rows_ref.shape[1])
    return jnp.concatenate(
        [jnp.dot(rows_ref[...], w[block, :], preferred_element_type=jnp.float32) for w in weight_refs], axis=0
    )


def tokens_kernel(drafts_ref, tokens_ref, arrived):
    copy = pltpu.make_async_copy(drafts_ref, tokens_ref, arrived)
    copy.start()
    copy.wait()


def own_kernel(hidden_ref, weight_ref, tokens_ref, parts_ref):
    logits = jnp.dot(hidden_ref[...], weight_ref[...], preferred_element_type=jnp.float32)
    me = lax.axis_index("dp")
    own_seqs = hidden_ref.shape[0] // POSITIONS
    shard = me * lax.axis_size("vocab") + lax.axis_index("vocab")
    totals, picks = contribution([(logits, shard)], tokens_ref[...], own_seqs, me * own_seqs, 0)
    for receiver in range(parts_ref.shape[0]):
        parts_ref[receiver] = parts_for(receiver, me, totals, picks)


def begin_kernel(rows_ref, weight_ref, other_ref, logits_ref):
    logits_ref[...] = product(rows_ref, (weight_ref, other_ref), 0, 0)


def add_kernel(piece, other_row, rows_ref, weight_ref, other_ref, before_ref, logits_ref):
    logits_ref[...] = before_ref[...] + product(rows_ref, (weight_ref, other_ref), piece, other_row)


def far_kernel(shift, late_ref, weight_ref, other_ref, logits_ref, tokens_ref, before_ref, parts_ref):
    rows = late_ref.shape[0]
    dp = before_ref.shape[0]
    copies = parts_ref.shape[0] // dp
    source = lax.rem(lax.axis_index("dp") + dp - shift, dp)
    core = lax.rem(lax.axis_index("vocab"), 2)
    shard = lax.axis_index("dp") * lax.axis_size("vocab") + lax.axis_index("vocab")
    logits = logits_ref[...] + product(late_ref, (weight_ref, other_ref), 2, 0)
    blocks = [(logits[:rows], shard), (logits[rows:], shard + 1 - 2 * core)]
    seqs = rows // POSITIONS
    totals, picks = contribution(blocks, tokens_ref[...], 2 * seqs, (2 * source + core) * seqs, core * seqs)
    for receiver in range(dp):
        part = before_ref[receiver] + parts_for(receiver, source, totals, picks)
        parts_ref[receiver * copies : (receiver + 1) * copies] = jnp.broadcast_to(part[None], (copies,) + part.shape)


def gather_rows(flat, starts, count):
    lines = flat.shape[0]
    lane = lax.broadcasted_iota(jnp.int32, (1, LANES), 1)
    out = []
    for low, high, start in starts:
        row = jnp.zeros((1, LANES), jnp.float32)
        for line in range(low // LANES, min(lines, (high - 1) // LANES + 1)):
            place = start - line * LANES
            moved = pltpu.roll(flat, lax.rem(lines * LANES - place, LANES), 1)[line : line + 1]
            row = jnp.where((lane + place >= 0) & (lane + place < LANES), moved, row)
        out.append(row[:, :count])
    return jnp.concatenate(out, axis=0)


def tail_kernel(seqs, parts_ref, cutoffs_ref, norm_ref, logprob_ref, expected_ref, loss_ref):
    own_seqs = cutoffs_ref.shape[1]
    flat = jnp.sum(parts_ref[...], axis=0)
    place = lax.broadcasted_iota(jnp.int32, flat.shape, 0) * LANES + lax.broadcasted_iota(jnp.int32, flat.shape, 1)
    log_total = jnp.log(jnp.where(place < POSITIONS * seqs, flat, 1.0))
    squares = jnp.sum(jnp.sum(log_total * log_total, axis=1, keepdims=True), axis=0, keepdims=True)
    loss_ref[...] = squares * (Z_WEIGHT / (seqs * POSITIONS))
    first = lax.axis_index("dp") * own_seqs
    ranges = [(p * seqs, (p + 1) * seqs, p * seqs + first) for p in range(POSITIONS)]
    log_norm = gather_rows(log_total, ranges, own_seqs)
    base = POSITIONS * seqs
    ranges = [(base + p * own_seqs, base + (p + 1) * own_seqs, base + p * own_seqs) for p in range(DRAFTS)]
    picks = gather_rows(flat, ranges, own_seqs)
    norm_ref[...] = log_norm
    logprob = picks - log_norm[:DRAFTS]
    logprob_ref[...] = logprob
    accept = jax.nn.sigmoid(logprob - cutoffs_ref[...].astype(jnp.float32) / 1024.0)
    product = accept[0:1]
    expected = product
    for p in range(1, DRAFTS):
        product = product * accept[p : p + 1]
        expected = expected + product
    expected_ref[...] = expected


def local(hidden, head_weight, drafts, cutoffs):
    dp, vocab = lax.axis_size("dp"), lax.axis_size("vocab")
    rows, depth = hidden.shape
    width = head_weight.shape[1]
    seqs, own_seqs = drafts.shape[0], rows // POSITIONS
    late_size = depth - 2 * RELAYED - EARLY
    half = rows // 2
    lines = payload_lines(seqs, own_seqs)
    params = pltpu.CompilerParams(vmem_limit_bytes=GRANT)
    cost = pl.CostEstimate(
        flops=2 * rows * depth * width, bytes_accessed=2 * depth * (rows + width), transcendentals=2 * rows * width
    )
    third_cost = pl.CostEstimate(
        flops=rows * depth * width // 2, bytes_accessed=depth * (rows + width) // 2, transcendentals=0
    )
    swap = [(i, i ^ 1) for i in range(vocab)]
    relay = [(i, i ^ 2) for i in range(vocab)]
    first_piece = pl.pallas_call(
        first_kernel,
        out_shape=jax.ShapeDtypeStruct((half, RELAYED), hidden.dtype),
        in_specs=[pl.BlockSpec(memory_space=pl.ANY)],
        out_specs=VMEM,
        scratch_shapes=[pltpu.SemaphoreType.DMA],
        cost_estimate=pl.CostEstimate(flops=HIDDEN_HINT, bytes_accessed=0, transcendentals=0),
        compiler_params=params,
        name="first_piece",
    )(pltpu.with_memory_space_constraint(hidden, pltpu.HBM))
    early_piece, late_piece = pl.pallas_call(
        pieces_kernel,
        out_shape=[jax.ShapeDtypeStruct((half, size), hidden.dtype) for size in (EARLY, late_size)],
        in_specs=[VMEM],
        out_specs=[VMEM] * 2,
        compiler_params=params,
        name="pieces",
    )(hidden)
    logits_shape = jax.ShapeDtypeStruct((rows, width), jnp.float32)
    for k in range(1, dp):
        shift = [(i, (i + k) % dp) for i in range(dp)]
        first = lax.ppermute(first_piece, "dp", shift)
        early = lax.ppermute(early_piece, "dp", shift)
        late = lax.ppermute(late_piece, "dp", shift)
        relayed = lax.ppermute(first, "vocab", relay)
        if k == 1:
            other_weight = lax.ppermute(head_weight, "vocab", swap)
            tokens = pl.pallas_call(
                tokens_kernel,
                out_shape=pltpu.VMEM((DRAFTS, seqs), drafts.dtype),
                in_specs=[pl.BlockSpec(memory_space=pl.ANY)],
                out_specs=VMEM,
                scratch_shapes=[pltpu.SemaphoreType.DMA],
                cost_estimate=pl.CostEstimate(flops=WEIGHT_HINT, bytes_accessed=0, transcendentals=0),
                compiler_params=params,
                name="tokens",
            )(pltpu.with_memory_space_constraint(drafts.T, pltpu.HBM))
            parts = pl.pallas_call(
                own_kernel,
                out_shape=jax.ShapeDtypeStruct((dp, lines, LANES), jnp.float32),
                in_specs=[VMEM] * 3,
                out_specs=VMEM,
                cost_estimate=cost,
                compiler_params=params,
                name="own_rows",
            )(hidden, head_weight, tokens)
        multiply = functools.partial(
            pl.pallas_call,
            out_shape=logits_shape,
            out_specs=VMEM,
            cost_estimate=third_cost,
            compiler_params=params,
        )
        call = multiply(begin_kernel, in_specs=[VMEM] * 3, name="begin")
        logits = call(first, head_weight, other_weight)
        call = multiply(functools.partial(add_kernel, 1, 0), in_specs=[VMEM] * 4, name="near")
        logits = call(early, head_weight, other_weight, logits)
        call = multiply(functools.partial(add_kernel, 0, 1), in_specs=[VMEM] * 4, name="middle")
        logits = call(relayed, head_weight, other_weight, logits)
        count = dp * vocab if k == dp - 1 else dp
        parts = pl.pallas_call(
            functools.partial(far_kernel, k),
            out_shape=jax.ShapeDtypeStruct((count, lines, LANES), jnp.float32),
            in_specs=[VMEM] * 6,
            out_specs=VMEM,
            cost_estimate=third_cost,
            compiler_params=params,
            name="far",
        )(late, head_weight, other_weight, logits, tokens, parts)
        if k < dp - 1:
            pieces = first_piece, early_piece, late_piece
            (first_piece, early_piece, late_piece), parts = lax.optimization_barrier((pieces, parts))
    parts = lax.all_to_all(parts, ("dp", "vocab"), 0, 0)
    log_norm, logprob, expected, loss = pl.pallas_call(
        functools.partial(tail_kernel, seqs),
        out_shape=(
            jax.ShapeDtypeStruct((POSITIONS, own_seqs), jnp.float32),
            jax.ShapeDtypeStruct((DRAFTS, own_seqs), jnp.float32),
            jax.ShapeDtypeStruct((1, own_seqs), jnp.float32),
            jax.ShapeDtypeStruct((1, 1), jnp.float32),
        ),
        in_specs=[VMEM] * 2,
        out_specs=(VMEM,) * 4,
        compiler_params=params,
        name="tail",
    )(parts, cutoffs.T)
    return log_norm.T, logprob.T, expected.reshape(own_seqs), loss.reshape(())


def solution(mesh):
    in_specs = (P("dp", None), P(None, ("dp", "vocab")), P(), P("dp", None))
    out_specs = (P("dp", None), P("dp", None), P("dp"), P())
    return jax.shard_map(local, mesh=mesh, in_specs=in_specs, out_specs=out_specs, check_vma=False)
```

```python
import functools

import jax
import jax.numpy as jnp
from jax import lax
from jax.experimental import pallas as pl
from jax.experimental.pallas import tpu as pltpu
from jax.sharding import PartitionSpec as P


DRAFTS = 4
POSITIONS = 5
SOFT_CAP = 30.0
Z_WEIGHT = 0.001
LANES = 128
SUBLANES = 8
GRANT = 16 * 2**20
RELAYED = 6 * LANES
EARLY = 9 * LANES
NEXT = 7 * LANES
HIDDEN_HINT = 1_200_000_000
WEIGHT_HINT = 3_000_000_000
VMEM = pl.BlockSpec(memory_space=pltpu.VMEM)
ANY = pl.BlockSpec(memory_space=pl.ANY)


def row_ids(drafts, rows, first_seq):
    shape = (rows, drafts.shape[1])
    seq = lax.broadcasted_iota(jnp.int32, shape, 1) - first_seq
    target = lax.broadcasted_iota(jnp.int32, shape, 0) - seq * POSITIONS
    shifted = (drafts + 1).astype(jnp.float32)
    picked = jnp.zeros(shape, jnp.float32)
    for p in range(DRAFTS):
        picked = jnp.where(target == p, shifted[p : p + 1], picked)
    return jnp.sum(picked, axis=1, keepdims=True).astype(jnp.int32) - 1


def spread(column, starts, lines):
    shape = (column.shape[0], LANES)
    offset = lax.broadcasted_iota(jnp.int32, shape, 0) - POSITIONS * lax.broadcasted_iota(jnp.int32, shape, 1)
    out = []
    for line in range(lines):
        values = jnp.zeros(shape, jnp.float32)
        for p, start in enumerate(starts):
            values = jnp.where(offset == POSITIONS * (line * LANES - start) + p, column, values)
        out.append(jnp.sum(values, axis=0, keepdims=True))
    return jnp.concatenate(out, axis=0)


def payload_lines(seqs, own_seqs):
    return -(-(POSITIONS * seqs + DRAFTS * own_seqs) // LANES)


def contribution(blocks, drafts, own_seqs, first_seq, local_seq):
    rows, width = blocks[0][0].shape
    seqs = drafts.shape[1]
    ids = row_ids(drafts, rows, first_seq)
    columns = lax.broadcasted_iota(jnp.int32, (rows, width), 1)
    totals = picks = 0.0
    for logits, shard in blocks:
        capped = SOFT_CAP * jnp.tanh(logits * (1.0 / SOFT_CAP))
        totals += jnp.exp(capped)
        picks += jnp.where(columns == ids - shard * width, capped, 0.0)
    totals = jnp.sum(totals, axis=1, keepdims=True)
    picks = jnp.sum(picks, axis=1, keepdims=True)
    lines = payload_lines(seqs, own_seqs)
    totals = spread(totals, [p * seqs + first_seq for p in range(POSITIONS)], lines)
    picks = spread(picks, [POSITIONS * seqs + p * own_seqs + local_seq for p in range(DRAFTS)], lines)
    return totals, picks


def parts_for(receiver, source, totals, picks):
    return totals + jnp.where(source == receiver, picks, 0.0)


def place(piece, other_row):
    if piece:
        return 2 * RELAYED + (0, EARLY, EARLY + NEXT)[piece - 1]
    row = lax.rem(lax.axis_index("vocab") // 2 + other_row, 2)
    return pl.multiple_of(row * RELAYED, LANES)


def half_start(rows):
    return pl.multiple_of(lax.rem(lax.axis_index("vocab"), 2) * rows, SUBLANES)


def first_kernel(hidden_ref, piece_ref, arrived):
    rows, size = piece_ref.shape
    source = hidden_ref.at[pl.ds(half_start(rows), rows), pl.ds(place(0, 0), size)]
    copy = pltpu.make_async_copy(source, piece_ref, arrived)
    copy.start()
    copy.wait()


def pieces_kernel(hidden_ref, *piece_refs):
    for piece, ref in enumerate(piece_refs, 1):
        rows, size = ref.shape
        ref[...] = hidden_ref[pl.ds(half_start(rows), rows), pl.ds(place(piece, 0), size)]


def product(rows_ref, weight_refs, piece, other_row):
    block = pl.ds(place(piece, other_row), rows_ref.shape[1])
    return jnp.concatenate(
        [jnp.dot(rows_ref[...], w[block, :], preferred_element_type=jnp.float32) for w in weight_refs], axis=0
    )


def tokens_kernel(drafts_ref, tokens_ref, arrived):
    copy = pltpu.make_async_copy(drafts_ref, tokens_ref, arrived)
    copy.start()
    copy.wait()


def own_kernel(hidden_ref, weight_ref, tokens_ref, parts_ref):
    logits = jnp.dot(hidden_ref[...], weight_ref[...], preferred_element_type=jnp.float32)
    me = lax.axis_index("dp")
    own_seqs = hidden_ref.shape[0] // POSITIONS
    shard = me * lax.axis_size("vocab") + lax.axis_index("vocab")
    totals, picks = contribution([(logits, shard)], tokens_ref[...], own_seqs, me * own_seqs, 0)
    for receiver in range(parts_ref.shape[0]):
        parts_ref[receiver] = parts_for(receiver, me, totals, picks)


def begin_kernel(rows_ref, weight_ref, other_ref, logits_ref):
    logits_ref[...] = product(rows_ref, (weight_ref, other_ref), 0, 0)


def add_kernel(piece, other_row, rows_ref, weight_ref, other_ref, before_ref, logits_ref):
    logits_ref[...] = before_ref[...] + product(rows_ref, (weight_ref, other_ref), piece, other_row)


def far_kernel(shift, late_ref, weight_ref, other_ref, logits_ref, tokens_ref, before_ref, parts_ref):
    rows = late_ref.shape[0]
    dp = before_ref.shape[0]
    copies = parts_ref.shape[0] // dp
    source = lax.rem(lax.axis_index("dp") + dp - shift, dp)
    core = lax.rem(lax.axis_index("vocab"), 2)
    shard = lax.axis_index("dp") * lax.axis_size("vocab") + lax.axis_index("vocab")
    logits = logits_ref[...] + product(late_ref, (weight_ref, other_ref), 3, 0)
    blocks = [(logits[:rows], shard), (logits[rows:], shard + 1 - 2 * core)]
    seqs = rows // POSITIONS
    totals, picks = contribution(blocks, tokens_ref[...], 2 * seqs, (2 * source + core) * seqs, core * seqs)
    for receiver in range(dp):
        part = before_ref[receiver] + parts_for(receiver, source, totals, picks)
        parts_ref[receiver * copies : (receiver + 1) * copies] = jnp.broadcast_to(part[None], (copies,) + part.shape)


def gather_rows(flat, starts, count):
    lines = flat.shape[0]
    lane = lax.broadcasted_iota(jnp.int32, (1, LANES), 1)
    out = []
    for low, high, start in starts:
        row = jnp.zeros((1, LANES), jnp.float32)
        for line in range(low // LANES, min(lines, (high - 1) // LANES + 1)):
            place = start - line * LANES
            moved = pltpu.roll(flat, lax.rem(lines * LANES - place, LANES), 1)[line : line + 1]
            row = jnp.where((lane + place >= 0) & (lane + place < LANES), moved, row)
        out.append(row[:, :count])
    return jnp.concatenate(out, axis=0)


def tail_kernel(seqs, parts_ref, cutoffs_ref, norm_ref, logprob_ref, expected_ref, loss_ref):
    own_seqs = cutoffs_ref.shape[1]
    flat = jnp.sum(parts_ref[...], axis=0)
    place = lax.broadcasted_iota(jnp.int32, flat.shape, 0) * LANES + lax.broadcasted_iota(jnp.int32, flat.shape, 1)
    log_total = jnp.log(jnp.where(place < POSITIONS * seqs, flat, 1.0))
    squares = jnp.sum(jnp.sum(log_total * log_total, axis=1, keepdims=True), axis=0, keepdims=True)
    loss_ref[...] = squares * (Z_WEIGHT / (seqs * POSITIONS))
    first = lax.axis_index("dp") * own_seqs
    ranges = [(p * seqs, (p + 1) * seqs, p * seqs + first) for p in range(POSITIONS)]
    log_norm = gather_rows(log_total, ranges, own_seqs)
    base = POSITIONS * seqs
    ranges = [(base + p * own_seqs, base + (p + 1) * own_seqs, base + p * own_seqs) for p in range(DRAFTS)]
    picks = gather_rows(flat, ranges, own_seqs)
    norm_ref[...] = log_norm
    logprob = picks - log_norm[:DRAFTS]
    logprob_ref[...] = logprob
    accept = jax.nn.sigmoid(logprob - cutoffs_ref[...].astype(jnp.float32) / 1024.0)
    product = accept[0:1]
    expected = product
    for p in range(1, DRAFTS):
        product = product * accept[p : p + 1]
        expected = expected + product
    expected_ref[...] = expected


def local(hidden, head_weight, drafts, cutoffs):
    dp, vocab = lax.axis_size("dp"), lax.axis_size("vocab")
    rows, depth = hidden.shape
    width = head_weight.shape[1]
    seqs, own_seqs = drafts.shape[0], rows // POSITIONS
    late_size = depth - 2 * RELAYED - EARLY - NEXT
    half = rows // 2
    lines = payload_lines(seqs, own_seqs)
    params = pltpu.CompilerParams(vmem_limit_bytes=GRANT)
    cost = pl.CostEstimate(
        flops=2 * rows * depth * width, bytes_accessed=2 * depth * (rows + width), transcendentals=2 * rows * width
    )
    third_cost = pl.CostEstimate(
        flops=rows * depth * width // 2, bytes_accessed=depth * (rows + width) // 2, transcendentals=0
    )
    swap = [(i, i ^ 1) for i in range(vocab)]
    relay = [(i, i ^ 2) for i in range(vocab)]
    first_piece = pl.pallas_call(
        first_kernel,
        out_shape=jax.ShapeDtypeStruct((half, RELAYED), hidden.dtype),
        in_specs=[pl.BlockSpec(memory_space=pl.ANY)],
        out_specs=VMEM,
        scratch_shapes=[pltpu.SemaphoreType.DMA],
        cost_estimate=pl.CostEstimate(flops=HIDDEN_HINT, bytes_accessed=0, transcendentals=0),
        compiler_params=params,
        name="first_piece",
    )(pltpu.with_memory_space_constraint(hidden, pltpu.HBM))
    early_piece, next_piece, late_piece = pl.pallas_call(
        pieces_kernel,
        out_shape=[jax.ShapeDtypeStruct((half, size), hidden.dtype) for size in (EARLY, NEXT, late_size)],
        in_specs=[VMEM],
        out_specs=[VMEM] * 3,
        compiler_params=params,
        name="pieces",
    )(hidden)
    logits_shape = jax.ShapeDtypeStruct((rows, width), jnp.float32)
    for k in range(1, dp):
        shift = [(i, (i + k) % dp) for i in range(dp)]
        first = lax.ppermute(first_piece, "dp", shift)
        early = lax.ppermute(early_piece, "dp", shift)
        following = lax.ppermute(next_piece, "dp", shift)
        late = lax.ppermute(late_piece, "dp", shift)
        relayed = lax.ppermute(first, "vocab", relay)
        if k == 1:
            other_weight = lax.ppermute(head_weight, "vocab", swap)
            tokens = pl.pallas_call(
                tokens_kernel,
                out_shape=pltpu.VMEM((DRAFTS, seqs), drafts.dtype),
                in_specs=[pl.BlockSpec(memory_space=pl.ANY)],
                out_specs=VMEM,
                scratch_shapes=[pltpu.SemaphoreType.DMA],
                cost_estimate=pl.CostEstimate(flops=WEIGHT_HINT, bytes_accessed=0, transcendentals=0),
                compiler_params=params,
                name="tokens",
            )(pltpu.with_memory_space_constraint(drafts.T, pltpu.HBM))
            parts = pl.pallas_call(
                own_kernel,
                out_shape=jax.ShapeDtypeStruct((dp, lines, LANES), jnp.float32),
                in_specs=[VMEM] * 3,
                out_specs=VMEM,
                cost_estimate=cost,
                compiler_params=params,
                name="own_rows",
            )(hidden, head_weight, tokens)
        multiply = functools.partial(
            pl.pallas_call,
            out_shape=logits_shape,
            out_specs=VMEM,
            cost_estimate=third_cost,
            compiler_params=params,
        )
        call = multiply(begin_kernel, in_specs=[VMEM] * 3, name="begin")
        logits = call(first, head_weight, other_weight)
        call = multiply(functools.partial(add_kernel, 1, 0), in_specs=[VMEM] * 4, name="near")
        logits = call(early, head_weight, other_weight, logits)
        call = multiply(functools.partial(add_kernel, 2, 0), in_specs=[VMEM] * 4, name="next")
        logits = call(following, head_weight, other_weight, logits)
        call = multiply(functools.partial(add_kernel, 0, 1), in_specs=[VMEM] * 4, name="middle")
        logits = call(relayed, head_weight, other_weight, logits)
        count = dp * vocab if k == dp - 1 else dp
        parts = pl.pallas_call(
            functools.partial(far_kernel, k),
            out_shape=jax.ShapeDtypeStruct((count, lines, LANES), jnp.float32),
            in_specs=[VMEM] * 6,
            out_specs=VMEM,
            cost_estimate=third_cost,
            compiler_params=params,
            name="far",
        )(late, head_weight, other_weight, logits, tokens, parts)
        if k < dp - 1:
            pieces = first_piece, early_piece, next_piece, late_piece
            (first_piece, early_piece, next_piece, late_piece), parts = lax.optimization_barrier((pieces, parts))
    parts = lax.all_to_all(parts, ("dp", "vocab"), 0, 0)
    log_norm, logprob, expected, loss = pl.pallas_call(
        functools.partial(tail_kernel, seqs),
        out_shape=(
            jax.ShapeDtypeStruct((POSITIONS, own_seqs), jnp.float32),
            jax.ShapeDtypeStruct((DRAFTS, own_seqs), jnp.float32),
            jax.ShapeDtypeStruct((1, own_seqs), jnp.float32),
            jax.ShapeDtypeStruct((1, 1), jnp.float32),
        ),
        in_specs=[VMEM] * 2,
        out_specs=(VMEM,) * 4,
        compiler_params=params,
        name="tail",
    )(parts, cutoffs.T)
    return log_norm.T, logprob.T, expected.reshape(own_seqs), loss.reshape(())


def solution(mesh):
    in_specs = (P("dp", None), P(None, ("dp", "vocab")), P(), P("dp", None))
    out_specs = (P("dp", None), P("dp", None), P("dp"), P())
    return jax.shard_map(local, mesh=mesh, in_specs=in_specs, out_specs=out_specs, check_vma=False)
```
